32 devices in a mesh: gx: 4 (over z), gy: 4 (over y, core), gz: 2 (over x).
Axes of the slice: x: 2, y: 2, z: 4, core: 2. Of those that a mesh axis runs over, the one named last changes fastest.
Arguments:
- gradients: bfloat16 [32, 768, 512], P(('gx', 'gy', 'gz')), may hold values from -6 to 6
- master_weights: float32 [768, 512], P(('gx', 'gy', 'gz')), may hold values from -10 to 10
- first_moment: float32 [768, 512], P(('gx', 'gy', 'gz')), may hold values from -8 to 8
- second_moment: float32 [768, 512], P(('gx', 'gy', 'gz')), may hold values from 1 to 100
- tensor_ids: int32 [768], P(('gx', 'gy', 'gz')), may hold values from 0 to 3, as said below
Outputs:
- new_master: float32 [768, 512], P(('gx', 'gy', 'gz'))
- new_first: float32 [768, 512], P(('gx', 'gy', 'gz'))
- new_second: float32 [768, 512], P(('gx', 'gy', 'gz'))
- scaled_update: float32 [768, 512], P(('gx', 'gy', 'gz'))
- params: bfloat16 [768, 512], replicated
The draws below stay inside these ranges and needn't reach their ends.
Inputs may be any that keep to these rules, and one draw needn't show every extreme that they name: `tensor_ids`: nondecreasing along the rows; every tensor of 4 owns one contiguous run of rows.
All inputs are finite; a program needn't handle non-finite values.
Results may differ from the reference program's by a relative error of at most 0.0045.
Values may be sent and summed in bfloat16 or wider, within the bound.
A program may use at most 64 MiB of HBM per device.

```python
import math
import jax
import jax.numpy as jnp
from jax import lax

COLS = 512
NT = 4
BROWS = 768
DEVICES = 32


def tensor_layout(key):
    base_rows = BROWS // NT
    spread = BROWS // (4 * NT)
    shifts = jax.random.randint(jax.random.fold_in(key, 11), (NT - 1,), -spread, spread + 1).astype(jnp.int32)
    leading = base_rows + shifts
    last_rows = (BROWS - jnp.sum(leading)).astype(jnp.int32)
    lengths = jnp.concatenate([leading, last_rows[None]])
    starts = jnp.cumsum(lengths) - lengths
    row_index = jnp.arange(BROWS, dtype=jnp.int32)
    tensor_ids = jnp.sum((row_index[:, None] >= starts[None, 1:]).astype(jnp.int32), axis=1).astype(jnp.int32)
    scales = jnp.exp(jax.random.uniform(jax.random.fold_in(key, 12), (NT,), jnp.float32, math.log(0.25), math.log(2.0)))
    return (tensor_ids, scales)


def draw_tensor_ids(key, part):
    tensor_ids, scales = tensor_layout(key)
    return tensor_ids


def draw_master_weights(key, part):
    tensor_ids, scales = tensor_layout(key)
    row_scale = scales[tensor_ids][:, None]
    values = jnp.clip(jax.random.normal(jax.random.fold_in(key, 13), (BROWS, COLS), jnp.float32), -5.0, 5.0)
    return (values * row_scale).astype(jnp.float32)


def strengthened(drawn, rng, source, target, parts, factor):
    owner, partner = [(jnp.arange(drawn.shape[axis_at]) // (drawn.shape[axis_at] // parts)).reshape([-1 if axis == axis_at else 1 for axis in range(drawn.ndim)]) for axis_at in (source, target)]
    chosen = jax.random.permutation(rng, parts)[partner]
    strong = (owner == chosen) | (owner == (partner + parts // 2) % parts)
    return jnp.where(strong, factor * drawn, drawn)


def levels(stream_key, dims, shards, low, top_value):
    factor_of, own = 1.0, jax.random.fold_in(stream_key, 6)
    for dim, blocks in shards:
        steps = jnp.exp(jax.random.uniform(jax.random.fold_in(own, dim), (blocks,), jnp.float32, low / len(shards), top_value / len(shards)))
        factor_of = factor_of * jnp.repeat(steps, dims[dim] // blocks).reshape([-1 if axis == dim else 1 for axis in range(len(dims))])
    return factor_of


def scatter_about(own_key, extent, deviation, most, split=(), kind=jnp.bfloat16):
    result = jax.random.normal(own_key, extent, jnp.float32) * deviation
    if len(split) > 0:
        result = levels(own_key, extent, split, -0.22, 0.18) * result
    return jnp.clip(result, min=-most, max=most).astype(kind)


def bell_draw_with(rng, shape, width, bound, pieces, heavy, kind=jnp.bfloat16):
    result = width * jax.random.normal(rng, shape, jnp.float32)
    if pieces:
        result = result * levels(rng, shape, pieces, -0.22, 0.18)
    return jnp.clip(strengthened(result, jax.random.fold_in(rng, 3), *heavy), -bound, bound).astype(kind)


def setup_inputs(seed: int = 0) -> dict:
    key_of = jax.random.split(jax.random.key(seed), 6)
    gradients = bell_draw_with(key_of[0], (DEVICES, BROWS, COLS), 1.0, 6.0, ((0, 32),), (0, 1, 32, 2.75))
    master_weights = draw_master_weights(jax.random.fold_in(key_of[5], 71), 0)
    first_moment = scatter_about(key_of[2], (BROWS, COLS), 2.0, 8.0, ((0, 32),), jnp.float32)
    second_moment = jnp.clip(jnp.exp(math.log(100.0) - 4.6051702 * jax.random.uniform(key_of[3], (BROWS, COLS), jnp.float32) ** levels(key_of[3], (BROWS, COLS), ((0, 32),), -0.2, 0.2)), 1.0, 100.0)
    tensor_ids = draw_tensor_ids(jax.random.fold_in(key_of[5], 71), 0)
    return {"gradients": gradients, "master_weights": master_weights, "first_moment": first_moment, "second_moment": second_moment, "tensor_ids": tensor_ids}


decay_first = 0.9
decay_second = 0.999
epsilon = 1e-06
weight_decay = 0.01
step_size = 0.05

def tensor_sums(values, onehot):
    return jnp.dot(lax.optimization_barrier(jnp.sum(values * values, axis=1)), onehot, precision=lax.Precision.HIGHEST)

def reference(gradients, master_weights, first_moment, second_moment, tensor_ids):
    summed = lax.optimization_barrier(jnp.sum(gradients.astype(jnp.float32), axis=0))
    new_first = decay_first * first_moment + (1.0 - decay_first) * summed
    new_second = decay_second * second_moment + (1.0 - decay_second) * summed * summed
    update = new_first / (jnp.sqrt(new_second) + epsilon) + weight_decay * master_weights
    onehot = (tensor_ids[:, None] == jnp.arange(NT, dtype=jnp.int32)[None, :]).astype(jnp.float32)
    weight_sq = tensor_sums(master_weights, onehot)
    update_sq = tensor_sums(update, onehot)
    counts = lax.optimization_barrier(jnp.sum(onehot, axis=0)) * COLS
    trust_ratio = jnp.sqrt(weight_sq / (update_sq + counts))
    row_trust = jnp.dot(onehot, trust_ratio, precision=lax.Precision.HIGHEST)
    scaled_update = row_trust[:, None] * update
    new_master = master_weights - step_size * scaled_update
    params = new_master.astype(jnp.bfloat16)
    return (new_master, new_first, new_second, scaled_update, params)
```

```python
import functools
import itertools

import jax
import jax.numpy as jnp
from jax import lax
from jax.experimental import pallas as pl
from jax.experimental.pallas import tpu as pltpu
from jax.sharding import PartitionSpec as P

NT = 4
MESH = pl.DeviceIdType.MESH

decay_first = 0.9
decay_second = 0.999
epsilon = 1e-06
weight_decay = 0.01
step_size = 0.05


def digits_of(extent):
    factors, base = [], 2
    while extent > 1:
        while extent % base == 0:
            factors.append(base)
            extent //= base
        base += 1
    return factors


def offset(index, amount, extent, sign=1):
    result, weight = 0, 1
    for base in digits_of(extent):
        step = (amount // weight) % base
        digit = index if weight == 1 else index // weight
        if weight * base < extent:
            digit = digit % base
        if step:
            digit = (digit + (step if sign > 0 else base - step)) % base
        result = result + weight * digit
        weight *= base
    return result


def kernel(
    sizes, grads, master, first, second, ids,
    out_master, out_first, out_second, out_scaled, out_params,
    own_half, far_half, pair_recv, pair_send, plane_recv, line_send, line_recv, acc,
    m_in, f_in, s_in, m_out, u_out, sums_send, sums_recv, gathered,
    load_own, load_far, load_small, pair_ss, pair_rs, plane_ss, plane_rs, line_ss, line_rs,
    sums_ss, sums_rs, gl_ss, gl_rs, gp_ss, gp_rs, gs_ss, gs_rs, store_sem, small_sem,
):
    A, Y, S, X = sizes
    rows, width = master.shape
    a = lax.axis_index("gx")
    gy = lax.axis_index("gy")
    x = lax.axis_index("gz")
    y, c = gy // S, gy % S

    def device(a_, y_, c_, x_):
        return (a_, y_ * S + c_, x_)

    def remote(src, dst, ss, rs, where):
        return pltpu.make_async_remote_copy(
            src_ref=src, dst_ref=dst, send_sem=ss, recv_sem=rs, device_id=device(*where), device_id_type=MESH
        )

    plane = [q for q in itertools.product(range(Y), range(X)) if q != (0, 0)]
    lines_far = list(range(A - 1, 0, -1))
    lines_near = list(range(1, A))
    others = [o for o in itertools.product(range(A), range(Y), range(S), range(X)) if o != (0, 0, 0, 0)]

    def at(da, dy, dc, dx, sign=1):
        return (offset(a, da, A, sign), offset(y, dy, Y, sign), offset(c, dc, S, sign), offset(x, dx, X, sign))

    barrier = pltpu.get_barrier_semaphore()
    for o in others:
        pl.semaphore_signal(barrier, inc=1, device_id=device(*at(*o)), device_id_type=MESH)

    loads_own, loads_far = {}, {}
    order = lines_far + [0]
    for d in order:
        target = offset(a, d, A)
        for k in range(1, S):
            loads_far[d, k] = pltpu.make_async_copy(
                grads.at[target, :, offset(c, k, S)], far_half.at[k - 1, d], load_far.at[k - 1, d]
            )
            loads_far[d, k].start()
    for d in order:
        target = offset(a, d, A)
        loads_own[d] = pltpu.make_async_copy(grads.at[target, :, c], own_half.at[d], load_own.at[d])
        loads_own[d].start()
    loads_small = [
        pltpu.make_async_copy(src, dst, load_small.at[i])
        for i, (src, dst) in enumerate(((master, m_in), (first, f_in), (second, s_in)))
    ]
    for copy in loads_small:
        copy.start()

    pl.semaphore_wait(barrier, len(others))

    sends = []
    pair = {}
    for d in order:
        for k in range(1, S):
            loads_far[d, k].wait()
            pair[d, k] = remote(
                far_half.at[k - 1, d], pair_recv.at[k - 1, d], pair_ss.at[k - 1, d], pair_rs.at[k - 1, d], at(0, 0, k, 0)
            )
            pair[d, k].start()

    ids_row = jnp.broadcast_to(ids[...], (rows, rows)).astype(jnp.float32)
    diagonal = lax.broadcasted_iota(jnp.int32, (rows, rows), 0) == lax.broadcasted_iota(jnp.int32, (rows, rows), 1)
    ids_col = jnp.sum(jnp.where(diagonal, ids_row, 0.0), axis=1, keepdims=True)
    lane = lax.broadcasted_iota(jnp.int32, (rows, 128), 1).astype(jnp.float32)
    hit_w, hit_u, hit_n = lane == ids_col, lane == ids_col + NT, lane == ids_col + 2 * NT
    for copy in loads_small:
        copy.wait()
    weights = m_in[...]
    weight_rows = jnp.sum(weights * weights, axis=1, keepdims=True)
    fixed_sums = jnp.where(hit_w, weight_rows, 0.0) + jnp.where(hit_n, float(width), 0.0)

    crossing = {}
    for d in order:
        loads_own[d].wait()
        for k in range(1, S):
            pair[d, k].wait_recv()
        for i, (dy, dx) in enumerate(plane):
            y_, x_ = offset(y, dy, Y), offset(x, dx, X)
            total = own_half[d, y_, x_].astype(jnp.float32)
            for k in range(1, S):
                total = total + pair_recv[k - 1, d, y_, x_].astype(jnp.float32)
            pair_send[d, i] = total.astype(jnp.bfloat16)
            crossing[d, i] = remote(
                pair_send.at[d, i], plane_recv.at[d, i], plane_ss.at[d, i], plane_rs.at[d, i], at(0, dy, 0, dx)
            )
            crossing[d, i].start()
        total = own_half[d, y, x].astype(jnp.float32)
        for k in range(1, S):
            total = total + pair_recv[k - 1, d, y, x].astype(jnp.float32)
        acc[d] = total

    along = {}
    for d in order:
        total = acc[d]
        for i in range(len(plane)):
            crossing[d, i].wait_recv()
            total = total + plane_recv[d, i].astype(jnp.float32)
        if d:
            line_send[d - 1] = total.astype(jnp.bfloat16)
            along[d] = remote(
                line_send.at[d - 1], line_recv.at[d - 1], line_ss.at[d - 1], line_rs.at[d - 1], at(d, 0, 0, 0)
            )
            along[d].start()
    summed = total
    for d in lines_near:
        along[d].wait_recv()
        summed = summed + line_recv[d - 1].astype(jnp.float32)

    new_first = decay_first * f_in[...] + (1.0 - decay_first) * summed
    new_second = decay_second * s_in[...] + (1.0 - decay_second) * summed * summed
    update = new_first / (jnp.sqrt(new_second) + epsilon) + weight_decay * weights
    update_rows = jnp.sum(update * update, axis=1, keepdims=True)
    own_sums = jnp.sum(fixed_sums + jnp.where(hit_u, update_rows, 0.0), axis=0, keepdims=True)
    sums_send[...] = own_sums
    exchange = []
    for i, o in enumerate(reversed(others)):
        exchange.append(remote(sums_send, sums_recv.at[i], sums_ss.at[i], sums_rs.at[i], at(*o)))
        exchange[-1].start()
    f_in[...] = new_first
    s_in[...] = new_second
    smalls = [
        pltpu.make_async_copy(f_in, out_first, small_sem.at[0]),
        pltpu.make_async_copy(s_in, out_second, small_sem.at[1]),
    ]
    for copy in smalls:
        copy.start()
    totals = own_sums
    for i in reversed(range(len(others))):
        exchange[i].wait_recv()
        totals = totals + sums_recv[i]
    row_totals = jnp.broadcast_to(totals, (rows, 128))
    row_weight, row_update, row_count = (
        jnp.sum(jnp.where(hit, row_totals, 0.0), axis=1, keepdims=True) for hit in (hit_w, hit_u, hit_n)
    )
    trust = jnp.sqrt(row_weight / (row_update + row_count))
    scaled = trust * update
    new_master = weights - step_size * scaled
    gathered[a, y, c, x] = new_master.astype(jnp.bfloat16)

    stores = []

    def store(where, slot):
        copy = pltpu.make_async_copy(gathered.at[where], out_params.at[where], store_sem.at[slot])
        copy.start()
        stores.append(copy)

    slots = iter(range(A * Y * S * X))
    own = (a, y, c, x)
    line_hops, plane_hops, core_hops = {}, {}, {}
    for d in lines_far:
        line_hops[d] = remote(gathered.at[own], gathered.at[own], gl_ss.at[d - 1], gl_rs.at[d - 1], at(d, 0, 0, 0))
        line_hops[d].start()

    def to_plane(d):
        block = at(d, 0, 0, 0, -1)
        for i, (dy, dx) in enumerate(plane):
            plane_hops[d, i] = remote(
                gathered.at[block], gathered.at[block], gp_ss.at[d, i], gp_rs.at[d, i], at(0, dy, 0, dx)
            )
            plane_hops[d, i].start()

    def to_cores(d, i, block):
        for k in range(1, S):
            core_hops[d, i, k] = remote(
                gathered.at[block], gathered.at[block], gs_ss.at[k - 1, d, i], gs_rs.at[k - 1, d, i], at(0, 0, k, 0)
            )
            core_hops[d, i, k].start()

    to_plane(0)
    to_cores(0, len(plane), own)
    m_out[...] = new_master
    u_out[...] = scaled
    for i, (src, dst) in enumerate(((m_out, out_master), (u_out, out_scaled))):
        smalls.append(pltpu.make_async_copy(src, dst, small_sem.at[2 + i]))
        smalls[-1].start()
    store(own, next(slots))
    for d in lines_near:
        line_hops[d].wait_recv()
        block = at(d, 0, 0, 0, -1)
        to_plane(d)
        to_cores(d, len(plane), block)
        store(block, next(slots))
    for d in [0] + lines_near:
        for i, (dy, dx) in enumerate(plane):
            plane_hops[d, i].wait_recv()
            block = at(d, dy, 0, dx, -1)
            to_cores(d, i, block)
            store(block, next(slots))
    for d in [0] + lines_near:
        for i, (dy, dx) in [(len(plane), (0, 0))] + list(enumerate(plane)):
            for k in range(1, S):
                core_hops[d, i, k].wait_recv()
                store(at(d, dy, k, dx, -1), next(slots))

    for group in (pair, crossing, along, line_hops, plane_hops, core_hops):
        for copy in group.values():
            copy.wait_send()
    for copy in exchange:
        copy.wait_send()
    for copy in stores + smalls:
        copy.wait()


def solution(mesh):
    A, gy, X = mesh.shape["gx"], mesh.shape["gy"], mesh.shape["gz"]
    S = 2 if gy % 2 == 0 else 1
    Y = gy // S
    total = A * gy * X
    planes = max(Y * X - 1, 1)
    lines = max(A - 1, 1)
    cores = max(S - 1, 1)
    bf16, f32 = jnp.bfloat16, jnp.float32
    dma = pltpu.SemaphoreType.DMA

    def on_device(gradients, master_weights, first_moment, second_moment, tensor_ids):
        rows, width = master_weights.shape
        anywhere = pl.BlockSpec(memory_space=pl.ANY)
        vmem = pltpu.VMEM
        small = jax.ShapeDtypeStruct((rows, width), f32)
        outs = pl.pallas_call(
            functools.partial(kernel, (A, Y, S, X)),
            out_shape=(small, small, small, small, jax.ShapeDtypeStruct((A, Y, S, X, rows, width), bf16)),
            in_specs=[anywhere] * 4 + [pl.BlockSpec(memory_space=vmem)],
            out_specs=(anywhere,) * 5,
            scratch_shapes=[
                vmem((A, Y, X, rows, width), bf16),
                vmem((cores, A, Y, X, rows, width), bf16),
                vmem((cores, A, Y, X, rows, width), bf16),
                vmem((A, planes, rows, width), bf16),
                vmem((A, planes, rows, width), bf16),
                vmem((lines, rows, width), bf16),
                vmem((lines, rows, width), bf16),
                vmem((A, rows, width), f32),
                vmem((rows, width), f32),
                vmem((rows, width), f32),
                vmem((rows, width), f32),
                vmem((rows, width), f32),
                vmem((rows, width), f32),
                vmem((1, 128), f32),
                vmem((max(total - 1, 1), 1, 128), f32),
                vmem((A, Y, S, X, rows, width), bf16),
                dma((A,)), dma((cores, A)), dma((3,)),
                dma((cores, A)), dma((cores, A)),
                dma((A, planes)), dma((A, planes)),
                dma((lines,)), dma((lines,)),
                dma((total,)), dma((total,)),
                dma((lines,)), dma((lines,)),
                dma((A, planes)), dma((A, planes)),
                dma((cores, A, planes + 1)), dma((cores, A, planes + 1)),
                dma((total,)), dma((4,)),
            ],
            compiler_params=pltpu.CompilerParams(collective_id=0, has_side_effects=True),
        )(
            gradients.reshape(A, Y, S, X, rows, width),
            master_weights,
            first_moment,
            second_moment,
            tensor_ids[None, :],
        )
        return (*outs[:4], outs[4].reshape(total * rows, width))

    axes = ("gx", "gy", "gz")
    return jax.shard_map(
        on_device,
        mesh=mesh,
        in_specs=(P(axes, None, None), P(axes, None), P(axes, None), P(axes, None), P(axes)),
        out_specs=(P(axes, None), P(axes, None), P(axes, None), P(axes, None), P()),
        check_vma=False,
    )
```

```python
import functools
import itertools

import jax
import jax.numpy as jnp
from jax import lax
from jax.experimental import pallas as pl
from jax.experimental.pallas import tpu as pltpu
from jax.sharding import PartitionSpec as P

NT = 4
MESH = pl.DeviceIdType.MESH

decay_first = 0.9
decay_second = 0.999
epsilon = 1e-06
weight_decay = 0.01
step_size = 0.05


def digits_of(extent):
    factors, base = [], 2
    while extent > 1:
        while extent % base == 0:
            factors.append(base)
            extent //= base
        base += 1
    return factors


def offset(index, amount, extent, sign=1):
    result, weight = 0, 1
    for base in digits_of(extent):
        step = (amount // weight) % base
        digit = index if weight == 1 else index // weight
        if weight * base < extent:
            digit = digit % base
        if step:
            digit = (digit + (step if sign > 0 else base - step)) % base
        result = result + weight * digit
        weight *= base
    return result


def kernel(
    sizes, grads, master, first, second, ids,
    m_out, first_out, second_out, u_out, gathered,
    own_half, far_half, pair_recv, pair_send, plane_recv, line_send, line_recv, acc,
    m_in, f_in, s_in, sums_send, sums_recv,
    load_own, load_far, load_small, pair_ss, pair_rs, plane_ss, plane_rs, line_ss, line_rs,
    sums_ss, sums_rs, gl_ss, gl_rs, gp_ss, gp_rs, gs_ss, gs_rs,
):
    A, Y, S, X = sizes
    rows, width = master.shape
    a = lax.axis_index("gx")
    gy = lax.axis_index("gy")
    x = lax.axis_index("gz")
    y, c = gy // S, gy % S

    def device(a_, y_, c_, x_):
        return (a_, y_ * S + c_, x_)

    def remote(src, dst, ss, rs, where):
        return pltpu.make_async_remote_copy(
            src_ref=src, dst_ref=dst, send_sem=ss, recv_sem=rs, device_id=device(*where), device_id_type=MESH
        )

    plane = [q for q in itertools.product(range(Y), range(X)) if q != (0, 0)]
    lines_far = list(range(A - 1, 0, -1))
    lines_near = list(range(1, A))
    others = [o for o in itertools.product(range(A), range(Y), range(S), range(X)) if o != (0, 0, 0, 0)]

    def at(da, dy, dc, dx, sign=1):
        return (offset(a, da, A, sign), offset(y, dy, Y, sign), offset(c, dc, S, sign), offset(x, dx, X, sign))

    barrier = pltpu.get_barrier_semaphore()
    for o in others:
        pl.semaphore_signal(barrier, inc=1, device_id=device(*at(*o)), device_id_type=MESH)

    loads_own, loads_far = {}, {}
    order = lines_far + [0]
    for d in order:
        target = offset(a, d, A)
        for k in range(1, S):
            loads_far[d, k] = pltpu.make_async_copy(
                grads.at[target, :, offset(c, k, S)], far_half.at[k - 1, d], load_far.at[k - 1, d]
            )
            loads_far[d, k].start()
    for d in order:
        target = offset(a, d, A)
        loads_own[d] = pltpu.make_async_copy(grads.at[target, :, c], own_half.at[d], load_own.at[d])
        loads_own[d].start()
    loads_small = [
        pltpu.make_async_copy(src, dst, load_small.at[i])
        for i, (src, dst) in enumerate(((master, m_in), (first, f_in), (second, s_in)))
    ]
    for copy in loads_small:
        copy.start()

    pl.semaphore_wait(barrier, len(others))

    sends = []
    pair = {}
    for d in order:
        for k in range(1, S):
            loads_far[d, k].wait()
            pair[d, k] = remote(
                far_half.at[k - 1, d], pair_recv.at[k - 1, d], pair_ss.at[k - 1, d], pair_rs.at[k - 1, d], at(0, 0, k, 0)
            )
            pair[d, k].start()

    ids_row = jnp.broadcast_to(ids[...], (rows, rows)).astype(jnp.float32)
    diagonal = lax.broadcasted_iota(jnp.int32, (rows, rows), 0) == lax.broadcasted_iota(jnp.int32, (rows, rows), 1)
    ids_col = jnp.sum(jnp.where(diagonal, ids_row, 0.0), axis=1, keepdims=True)
    lane = lax.broadcasted_iota(jnp.int32, (rows, 128), 1).astype(jnp.float32)
    hit_w, hit_u, hit_n = lane == ids_col, lane == ids_col + NT, lane == ids_col + 2 * NT
    for copy in loads_small:
        copy.wait()
    weights = m_in[...]
    weight_rows = jnp.sum(weights * weights, axis=1, keepdims=True)
    fixed_sums = jnp.where(hit_w, weight_rows, 0.0) + jnp.where(hit_n, float(width), 0.0)

    crossing = {}
    for d in order:
        loads_own[d].wait()
        for k in range(1, S):
            pair[d, k].wait_recv()
        for i, (dy, dx) in enumerate(plane):
            y_, x_ = offset(y, dy, Y), offset(x, dx, X)
            total = own_half[d, y_, x_].astype(jnp.float32)
            for k in range(1, S):
                total = total + pair_recv[k - 1, d, y_, x_].astype(jnp.float32)
            pair_send[d, i] = total.astype(jnp.bfloat16)
            crossing[d, i] = remote(
                pair_send.at[d, i], plane_recv.at[d, i], plane_ss.at[d, i], plane_rs.at[d, i], at(0, dy, 0, dx)
            )
            crossing[d, i].start()
        total = own_half[d, y, x].astype(jnp.float32)
        for k in range(1, S):
            total = total + pair_recv[k - 1, d, y, x].astype(jnp.float32)
        acc[d] = total

    along = {}
    for d in order:
        total = acc[d]
        for i in range(len(plane)):
            crossing[d, i].wait_recv()
            total = total + plane_recv[d, i].astype(jnp.float32)
        if d:
            line_send[d - 1] = total.astype(jnp.bfloat16)
            along[d] = remote(
                line_send.at[d - 1], line_recv.at[d - 1], line_ss.at[d - 1], line_rs.at[d - 1], at(d, 0, 0, 0)
            )
            along[d].start()
    summed = total
    for d in lines_near:
        along[d].wait_recv()
        summed = summed + line_recv[d - 1].astype(jnp.float32)

    new_first = decay_first * f_in[...] + (1.0 - decay_first) * summed
    new_second = decay_second * s_in[...] + (1.0 - decay_second) * summed * summed
    update = new_first / (jnp.sqrt(new_second) + epsilon) + weight_decay * weights
    update_rows = jnp.sum(update * update, axis=1, keepdims=True)
    own_sums = jnp.sum(fixed_sums + jnp.where(hit_u, update_rows, 0.0), axis=0, keepdims=True)
    sums_send[...] = own_sums
    exchange = []
    for i, o in enumerate(reversed(others)):
        exchange.append(remote(sums_send, sums_recv.at[i], sums_ss.at[i], sums_rs.at[i], at(*o)))
        exchange[-1].start()
    first_out[...] = new_first
    second_out[...] = new_second
    totals = own_sums
    for i in reversed(range(len(others))):
        exchange[i].wait_recv()
        totals = totals + sums_recv[i]
    row_totals = jnp.broadcast_to(totals, (rows, 128))
    row_weight, row_update, row_count = (
        jnp.sum(jnp.where(hit, row_totals, 0.0), axis=1, keepdims=True) for hit in (hit_w, hit_u, hit_n)
    )
    trust = jnp.sqrt(row_weight / (row_update + row_count))
    scaled = trust * update
    new_master = weights - step_size * scaled
    gathered[a, y, c, x] = new_master.astype(jnp.bfloat16)

    own = (a, y, c, x)
    line_hops, plane_hops, core_hops = {}, {}, {}
    for d in lines_far:
        line_hops[d] = remote(gathered.at[own], gathered.at[own], gl_ss.at[d - 1], gl_rs.at[d - 1], at(d, 0, 0, 0))
        line_hops[d].start()

    def to_plane(d):
        block = at(d, 0, 0, 0, -1)
        for i, (dy, dx) in enumerate(plane):
            plane_hops[d, i] = remote(
                gathered.at[block], gathered.at[block], gp_ss.at[d, i], gp_rs.at[d, i], at(0, dy, 0, dx)
            )
            plane_hops[d, i].start()

    def to_cores(d, i, block):
        for k in range(1, S):
            core_hops[d, i, k] = remote(
                gathered.at[block], gathered.at[block], gs_ss.at[k - 1, d, i], gs_rs.at[k - 1, d, i], at(0, 0, k, 0)
            )
            core_hops[d, i, k].start()

    to_plane(0)
    to_cores(0, len(plane), own)
    m_out[...] = new_master
    u_out[...] = scaled
    for d in lines_near:
        line_hops[d].wait_recv()
        block = at(d, 0, 0, 0, -1)
        to_plane(d)
        to_cores(d, len(plane), block)
    for d in [0] + lines_near:
        for i, (dy, dx) in enumerate(plane):
            plane_hops[d, i].wait_recv()
            block = at(d, dy, 0, dx, -1)
            to_cores(d, i, block)
    for d in [0] + lines_near:
        for i, (dy, dx) in [(len(plane), (0, 0))] + list(enumerate(plane)):
            for k in range(1, S):
                core_hops[d, i, k].wait_recv()

    for group in (pair, crossing, along, line_hops, plane_hops, core_hops):
        for copy in group.values():
            copy.wait_send()
    for copy in exchange:
        copy.wait_send()


def write_out(*refs):
    count = len(refs) // 2
    sems = refs[-1]
    copies = [pltpu.make_async_copy(refs[i], refs[count + i], sems.at[i]) for i in range(count)]
    for copy in reversed(copies):
        copy.start()
    for copy in copies:
        copy.wait()


def solution(mesh):
    A, gy, X = mesh.shape["gx"], mesh.shape["gy"], mesh.shape["gz"]
    S = 2 if gy % 2 == 0 else 1
    Y = gy // S
    total = A * gy * X
    planes = max(Y * X - 1, 1)
    lines = max(A - 1, 1)
    cores = max(S - 1, 1)
    bf16, f32 = jnp.bfloat16, jnp.float32
    dma = pltpu.SemaphoreType.DMA

    def on_device(gradients, master_weights, first_moment, second_moment, tensor_ids):
        rows, width = master_weights.shape
        anywhere = pl.BlockSpec(memory_space=pl.ANY)
        vmem = pltpu.VMEM
        small = jax.ShapeDtypeStruct((rows, width), f32)
        outs = pl.pallas_call(
            functools.partial(kernel, (A, Y, S, X)),
            out_shape=(vmem((rows, width), f32),) * 4 + (vmem((A, Y, S, X, rows, width), bf16),),
            in_specs=[anywhere] * 4 + [pl.BlockSpec(memory_space=vmem)],
            out_specs=(pl.BlockSpec(memory_space=vmem),) * 5,
            scratch_shapes=[
                vmem((A, Y, X, rows, width), bf16),
                vmem((cores, A, Y, X, rows, width), bf16),
                vmem((cores, A, Y, X, rows, width), bf16),
                vmem((A, planes, rows, width), bf16),
                vmem((A, planes, rows, width), bf16),
                vmem((lines, rows, width), bf16),
                vmem((lines, rows, width), bf16),
                vmem((A, rows, width), f32),
                vmem((rows, width), f32),
                vmem((rows, width), f32),
                vmem((rows, width), f32),
                vmem((1, 128), f32),
                vmem((max(total - 1, 1), 1, 128), f32),
                dma((A,)), dma((cores, A)), dma((3,)),
                dma((cores, A)), dma((cores, A)),
                dma((A, planes)), dma((A, planes)),
                dma((lines,)), dma((lines,)),
                dma((total,)), dma((total,)),
                dma((lines,)), dma((lines,)),
                dma((A, planes)), dma((A, planes)),
                dma((cores, A, planes + 1)), dma((cores, A, planes + 1)),
            ],
            compiler_params=pltpu.CompilerParams(collective_id=0, has_side_effects=True),
        )(
            gradients.reshape(A, Y, S, X, rows, width),
            master_weights,
            first_moment,
            second_moment,
            tensor_ids[None, :],
        )
        written = pl.pallas_call(
            write_out,
            out_shape=(small,) * 4 + (jax.ShapeDtypeStruct((A, Y, S, X, rows, width), bf16),),
            in_specs=[pl.BlockSpec(memory_space=vmem)] * 5,
            out_specs=(anywhere,) * 5,
            scratch_shapes=[dma((5,))],
        )(*(pltpu.with_memory_space_constraint(out, vmem) for out in outs))
        return (*written[:4], written[4].reshape(total * rows, width))

    axes = ("gx", "gy", "gz")
    return jax.shard_map(
        on_device,
        mesh=mesh,
        in_specs=(P(axes, None, None), P(axes, None), P(axes, None), P(axes, None), P(axes)),
        out_specs=(P(axes, None), P(axes, None), P(axes, None), P(axes, None), P()),
        check_vma=False,
    )
```

```python
import functools
import itertools

import jax
import jax.numpy as jnp
from jax import lax
from jax.experimental import pallas as pl
from jax.experimental.pallas import tpu as pltpu
from jax.sharding import PartitionSpec as P

NT = 4
MESH = pl.DeviceIdType.MESH
VMEM_BYTES = 67043328
LARGEST_GRANT = 60 * 1024 * 1024

decay_first = 0.9
decay_second = 0.999
epsilon = 1e-06
weight_decay = 0.01
step_size = 0.05


def digits_of(extent):
    factors, base = [], 2
    while extent > 1:
        while extent % base == 0:
            factors.append(base)
            extent //= base
        base += 1
    return factors


def offset(index, amount, extent, sign=1):
    result, weight = 0, 1
    for base in digits_of(extent):
        step = (amount // weight) % base
        digit = index if weight == 1 else index // weight
        if weight * base < extent:
            digit = digit % base
        if step:
            digit = (digit + (step if sign > 0 else base - step)) % base
        result = result + weight * digit
        weight *= base
    return result


def kernel(
    sizes, grads, master, first, second, ids,
    m_out, first_out, second_out, u_out, all_master, all_update, totals_out,
    own_half, far_half, pair_recv, pair_send, plane_recv, line_send, line_recv, acc,
    m_in, f_in, s_in, line_sums, plane_sums, core_sums,
    load_own, load_far, load_small, pair_ss, pair_rs, plane_ss, plane_rs, line_ss, line_rs,
    sl_ss, sl_rs, sp_ss, sp_rs, sc_ss, sc_rs,
    ml_ss, ml_rs, mp_ss, mp_rs, mc_ss, mc_rs, ul_ss, ul_rs, up_ss, up_rs, uc_ss, uc_rs,
):
    A, Y, S, X = sizes
    rows, width = master.shape
    a = lax.axis_index("gx")
    gy = lax.axis_index("gy")
    x = lax.axis_index("gz")
    y, c = gy // S, gy % S

    def device(a_, y_, c_, x_):
        return (a_, y_ * S + c_, x_)

    def remote(src, dst, ss, rs, where):
        return pltpu.make_async_remote_copy(
            src_ref=src, dst_ref=dst, send_sem=ss, recv_sem=rs, device_id=device(*where), device_id_type=MESH
        )

    plane = [q for q in itertools.product(range(Y), range(X)) if q != (0, 0)]
    lines_far = list(range(A - 1, 0, -1))
    lines_near = list(range(1, A))
    others = [(d, 0, 0, 0) for d in lines_far] + [(0, dy, 0, dx) for dy, dx in plane] + [(0, 0, k, 0) for k in range(1, S)]

    def at(da, dy, dc, dx, sign=1):
        return (offset(a, da, A, sign), offset(y, dy, Y, sign), offset(c, dc, S, sign), offset(x, dx, X, sign))

    barrier = pltpu.get_barrier_semaphore()
    for o in others:
        pl.semaphore_signal(barrier, inc=1, device_id=device(*at(*o)), device_id_type=MESH)

    loads_own, loads_far = {}, {}
    order = lines_far + [0]
    for d in order:
        target = offset(a, d, A)
        for k in range(1, S):
            loads_far[d, k] = pltpu.make_async_copy(
                grads.at[target, :, offset(c, k, S)], far_half.at[k - 1, d], load_far.at[k - 1, d]
            )
            loads_far[d, k].start()
    for d in order:
        target = offset(a, d, A)
        loads_own[d] = pltpu.make_async_copy(grads.at[target, :, c], own_half.at[d], load_own.at[d])
        loads_own[d].start()
    loads_small = [
        pltpu.make_async_copy(src, dst, load_small.at[i])
        for i, (src, dst) in enumerate(((master, m_in), (first, f_in), (second, s_in)))
    ]
    for copy in loads_small:
        copy.start()

    pl.semaphore_wait(barrier, len(others))

    own = (a, y, c, x)

    class Gather:
        def __init__(self, ref, line_sems, plane_sems, core_sems):
            self.ref, self.line_sems, self.plane_sems, self.core_sems = ref, line_sems, plane_sems, core_sems
            self.line, self.plane, self.core = {}, {}, {}

        def copy(self, block, sems, slot, where):
            ref = self.ref.at[block]
            hop = remote(ref, ref, sems[0].at[slot], sems[1].at[slot], at(*where))
            hop.start()
            return hop

        def to_line(self):
            for d in lines_far:
                self.line[d] = self.copy(own, self.line_sems, d - 1, (d, 0, 0, 0))

        def to_plane(self, d):
            for i, (dy, dx) in enumerate(plane):
                self.plane[d, i] = self.copy(at(d, 0, 0, 0, -1), self.plane_sems, (d, i), (0, dy, 0, dx))

        def to_core(self, d, i):
            dy, dx = plane[i] if i < len(plane) else (0, 0)
            for k in range(1, S):
                self.core[d, i, k] = self.copy(at(d, dy, 0, dx, -1), self.core_sems, (k - 1, d, i), (0, 0, k, 0))

        def relay_line(self, d):
            self.line[d].wait_recv()
            self.to_plane(d)
            self.to_core(d, len(plane))

        def relay_plane(self, d):
            for i in range(len(plane)):
                self.plane[d, i].wait_recv()
                self.to_core(d, i)

        def finish(self):
            for hop in self.core.values():
                hop.wait_recv()
            for group in (self.line, self.plane, self.core):
                for hop in group.values():
                    hop.wait_send()

    of_master = Gather(all_master, (ml_ss, ml_rs), (mp_ss, mp_rs), (mc_ss, mc_rs))
    of_update = Gather(all_update, (ul_ss, ul_rs), (up_ss, up_rs), (uc_ss, uc_rs))

    pair = {}
    for d in order:
        for k in range(1, S):
            loads_far[d, k].wait()
            pair[d, k] = remote(
                far_half.at[k - 1, d], pair_recv.at[k - 1, d], pair_ss.at[k - 1, d], pair_rs.at[k - 1, d], at(0, 0, k, 0)
            )
            pair[d, k].start()

    ids_row = jnp.broadcast_to(ids[...], (rows, rows)).astype(jnp.float32)
    diagonal = lax.broadcasted_iota(jnp.int32, (rows, rows), 0) == lax.broadcasted_iota(jnp.int32, (rows, rows), 1)
    ids_col = jnp.sum(jnp.where(diagonal, ids_row, 0.0), axis=1, keepdims=True)
    lane = lax.broadcasted_iota(jnp.int32, (rows, 128), 1).astype(jnp.float32)
    hit_w, hit_u, hit_n = lane == ids_col, lane == ids_col + NT, lane == ids_col + 2 * NT
    for copy in loads_small:
        copy.wait()
    weights = m_in[...]
    all_master[own] = weights.astype(jnp.bfloat16)
    of_master.to_line()
    of_master.to_plane(0)
    of_master.to_core(0, len(plane))
    weight_rows = jnp.sum(weights * weights, axis=1, keepdims=True)
    fixed_sums = jnp.where(hit_w, weight_rows, 0.0) + jnp.where(hit_n, float(width), 0.0)

    crossing = {}
    for d in order:
        loads_own[d].wait()
        for k in range(1, S):
            pair[d, k].wait_recv()
        for i, (dy, dx) in enumerate(plane):
            y_, x_ = offset(y, dy, Y), offset(x, dx, X)
            total = own_half[d, y_, x_].astype(jnp.float32)
            for k in range(1, S):
                total = total + pair_recv[k - 1, d, y_, x_].astype(jnp.float32)
            pair_send[d, i] = total.astype(jnp.bfloat16)
            crossing[d, i] = remote(
                pair_send.at[d, i], plane_recv.at[d, i], plane_ss.at[d, i], plane_rs.at[d, i], at(0, dy, 0, dx)
            )
            crossing[d, i].start()
        total = own_half[d, y, x].astype(jnp.float32)
        for k in range(1, S):
            total = total + pair_recv[k - 1, d, y, x].astype(jnp.float32)
        acc[d] = total

    along = {}
    for d in order:
        if d == 0:
            for near in lines_near:
                of_master.relay_line(near)
        total = acc[d]
        for i in range(len(plane)):
            crossing[d, i].wait_recv()
            total = total + plane_recv[d, i].astype(jnp.float32)
        if d:
            line_send[d - 1] = total.astype(jnp.bfloat16)
            along[d] = remote(
                line_send.at[d - 1], line_recv.at[d - 1], line_ss.at[d - 1], line_rs.at[d - 1], at(d, 0, 0, 0)
            )
            along[d].start()
    summed = total
    for d in lines_near:
        along[d].wait_recv()
        summed = summed + line_recv[d - 1].astype(jnp.float32)

    new_first = decay_first * f_in[...] + (1.0 - decay_first) * summed
    new_second = decay_second * s_in[...] + (1.0 - decay_second) * summed * summed
    update = new_first / (jnp.sqrt(new_second) + epsilon) + weight_decay * weights
    update_rows = jnp.sum(update * update, axis=1, keepdims=True)
    own_sums = jnp.sum(fixed_sums + jnp.where(hit_u, update_rows, 0.0), axis=0, keepdims=True)
    line_sums[a] = own_sums
    hops = []

    def send_sums(ref, mine, sems, slot, where):
        hops.append(remote(ref.at[mine], ref.at[mine], sems[0].at[slot], sems[1].at[slot], at(*where)))
        hops[-1].start()
        return hops[-1]

    sums_line = [send_sums(line_sums, a, (sl_ss, sl_rs), d - 1, (d, 0, 0, 0)) for d in lines_far]
    all_update[own] = update.astype(jnp.bfloat16)
    of_update.to_line()
    of_update.to_plane(0)
    of_update.to_core(0, len(plane))
    first_out[...] = new_first
    second_out[...] = new_second
    for d in [0] + lines_near:
        of_master.relay_plane(d)
    for d in lines_near[:-1]:
        of_update.relay_line(d)
    for hop in sums_line:
        hop.wait_recv()
    subtotal = line_sums[0]
    for i in range(1, A):
        subtotal = subtotal + line_sums[i]
    here = y * X + x
    plane_sums[here] = subtotal
    sums_plane = [
        send_sums(plane_sums, here, (sp_ss, sp_rs), i, (0, dy, 0, dx)) for i, (dy, dx) in enumerate(plane)
    ]
    for d in lines_near[-1:]:
        of_update.relay_line(d)
    of_update.relay_plane(0)
    for hop in sums_plane:
        hop.wait_recv()
    subtotal = plane_sums[0]
    for i in range(1, Y * X):
        subtotal = subtotal + plane_sums[i]
    core_sums[c] = subtotal
    sums_core = [send_sums(core_sums, c, (sc_ss, sc_rs), k - 1, (0, 0, k, 0)) for k in range(1, S)]
    for d in lines_near[:-1]:
        of_update.relay_plane(d)
    for hop in sums_core:
        hop.wait_recv()
    totals = core_sums[0]
    for i in range(1, S):
        totals = totals + core_sums[i]
    totals_out[...] = totals
    row_totals = jnp.broadcast_to(totals, (rows, 128))
    row_weight, row_update, row_count = (
        jnp.sum(jnp.where(hit, row_totals, 0.0), axis=1, keepdims=True) for hit in (hit_w, hit_u, hit_n)
    )
    trust = jnp.sqrt(row_weight / (row_update + row_count))
    scaled = trust * update
    m_out[...] = weights - step_size * scaled
    u_out[...] = scaled
    for d in lines_near[-1:]:
        of_update.relay_plane(d)
    of_master.finish()
    of_update.finish()
    for group in (pair, crossing, along):
        for copy in group.values():
            copy.wait_send()
    for hop in hops:
        hop.wait_send()


def write_out(sizes, all_master, all_update, totals, *refs):
    A, Y, S, X = sizes
    rows, width = all_master.shape[-2:]
    kept, out_kept, out_params, params, sems, param_sems = refs[:4], refs[4:8], refs[8], refs[9], refs[10], refs[11]
    copies = [pltpu.make_async_copy(kept[i], out_kept[i], sems.at[i]) for i in range(4)]
    for copy in copies:
        copy.start()
    values = totals[...]
    weight_sq, update_sq, counts = (
        [values[:, group * NT + t : group * NT + t + 1] for t in range(NT)] for group in range(3)
    )
    steps = [step_size * jnp.sqrt(weight_sq[t] / (update_sq[t] + counts[t])) for t in range(NT)]
    ends, end = [], 0.0
    for t in range(NT - 1):
        end = end + counts[t]
        ends.append(end)
    row_of = lax.broadcasted_iota(jnp.int32, (rows, 1), 0)
    for i in range(A):
        for j, (y, c, x) in enumerate(itertools.product(range(Y), range(S), range(X))):
            block = i * Y * S * X + j
            place = ((row_of + block * rows) * width).astype(jnp.float32)
            step = jnp.broadcast_to(steps[NT - 1], (rows, 1))
            for t in reversed(range(NT - 1)):
                step = jnp.where(place < ends[t], steps[t], step)
            value = all_master[i, y, c, x].astype(jnp.float32) - step * all_update[i, y, c, x].astype(jnp.float32)
            params[i, y, c, x] = value.astype(jnp.bfloat16)
        copies.append(pltpu.make_async_copy(params.at[i], out_params.at[i], param_sems.at[i]))
        copies[-1].start()
    for copy in copies:
        copy.wait()


def solution(mesh):
    A, gy, X = mesh.shape["gx"], mesh.shape["gy"], mesh.shape["gz"]
    S = 2 if gy % 2 == 0 else 1
    Y = gy // S
    total = A * gy * X
    planes = max(Y * X - 1, 1)
    lines = max(A - 1, 1)
    cores = max(S - 1, 1)
    bf16, f32 = jnp.bfloat16, jnp.float32
    dma = pltpu.SemaphoreType.DMA

    def on_device(gradients, master_weights, first_moment, second_moment, tensor_ids):
        rows, width = master_weights.shape
        anywhere = pl.BlockSpec(memory_space=pl.ANY)
        vmem = pltpu.VMEM
        small = jax.ShapeDtypeStruct((rows, width), f32)
        kept_bytes = rows * width * 4 * (total + 4) + 1024 * 1024
        grant = min(LARGEST_GRANT, VMEM_BYTES - kept_bytes)
        outs = pl.pallas_call(
            functools.partial(kernel, (A, Y, S, X)),
            out_shape=(vmem((rows, width), f32),) * 4 + (vmem((A, Y, S, X, rows, width), bf16),) * 2 + (vmem((1, 128), f32),),
            in_specs=[anywhere] * 4 + [pl.BlockSpec(memory_space=vmem)],
            out_specs=(pl.BlockSpec(memory_space=vmem),) * 7,
            scratch_shapes=[
                vmem((A, Y, X, rows, width), bf16),
                vmem((cores, A, Y, X, rows, width), bf16),
                vmem((cores, A, Y, X, rows, width), bf16),
                vmem((A, planes, rows, width), bf16),
                vmem((A, planes, rows, width), bf16),
                vmem((lines, rows, width), bf16),
                vmem((lines, rows, width), bf16),
                vmem((A, rows, width), f32),
                vmem((rows, width), f32),
                vmem((rows, width), f32),
                vmem((rows, width), f32),
                vmem((A, 1, 128), f32),
                vmem((Y * X, 1, 128), f32),
                vmem((S, 1, 128), f32),
                dma((A,)), dma((cores, A)), dma((3,)),
                dma((cores, A)), dma((cores, A)),
                dma((A, planes)), dma((A, planes)),
                dma((lines,)), dma((lines,)),
                dma((lines,)), dma((lines,)), dma((planes,)), dma((planes,)), dma((cores,)), dma((cores,)),
                dma((lines,)), dma((lines,)), dma((A, planes)), dma((A, planes)),
                dma((cores, A, planes + 1)), dma((cores, A, planes + 1)),
                dma((lines,)), dma((lines,)), dma((A, planes)), dma((A, planes)),
                dma((cores, A, planes + 1)), dma((cores, A, planes + 1)),
            ],
            compiler_params=pltpu.CompilerParams(collective_id=0, has_side_effects=True, vmem_limit_bytes=grant),
        )(
            gradients.reshape(A, Y, S, X, rows, width),
            master_weights,
            first_moment,
            second_moment,
            tensor_ids[None, :],
        )
        outs = [pltpu.with_memory_space_constraint(out, vmem) for out in outs]
        written = pl.pallas_call(
            functools.partial(write_out, (A, Y, S, X)),
            out_shape=(small,) * 4 + (jax.ShapeDtypeStruct((A, Y, S, X, rows, width), bf16),),
            in_specs=[pl.BlockSpec(memory_space=vmem)] * 7,
            out_specs=(anywhere,) * 5,
            scratch_shapes=[vmem((A, Y, S, X, rows, width), bf16), dma((4,)), dma((A,))],
            compiler_params=pltpu.CompilerParams(vmem_limit_bytes=grant),
        )(outs[4], outs[5], outs[6], outs[0], outs[1], outs[2], outs[3])
        return (*written[:4], written[4].reshape(total * rows, width))

    axes = ("gx", "gy", "gz")
    return jax.shard_map(
        on_device,
        mesh=mesh,
        in_specs=(P(axes, None, None), P(axes, None), P(axes, None), P(axes, None), P(axes)),
        out_specs=(P(axes, None), P(axes, None), P(axes, None), P(axes, None), P()),
        check_vma=False,
    )
```

```python
import functools
import itertools

import jax
import jax.numpy as jnp
from jax import lax
from jax.experimental import pallas as pl
from jax.experimental.pallas import tpu as pltpu
from jax.sharding import PartitionSpec as P

NT = 4
MESH = pl.DeviceIdType.MESH
VMEM_BYTES = 67043328
LARGEST_GRANT = 60 * 1024 * 1024

decay_first = 0.9
decay_second = 0.999
epsilon = 1e-06
weight_decay = 0.01
step_size = 0.05


def digits_of(extent):
    factors, base = [], 2
    while extent > 1:
        while extent % base == 0:
            factors.append(base)
            extent //= base
        base += 1
    return factors


def offset(index, amount, extent, sign=1):
    result, weight = 0, 1
    for base in digits_of(extent):
        step = (amount // weight) % base
        digit = index if weight == 1 else index // weight
        if weight * base < extent:
            digit = digit % base
        if step:
            digit = (digit + (step if sign > 0 else base - step)) % base
        result = result + weight * digit
        weight *= base
    return result


def kernel(
    sizes, grads, master, first, second, ids,
    m_out, first_out, second_out, u_out, all_master, all_update, totals_out,
    own_half, far_half, pair_recv, pair_send, plane_recv, line_send, line_recv, acc,
    m_in, f_in, s_in, line_sums, plane_sums, core_sums,
    load_own, load_far, load_small, pair_ss, pair_rs, plane_ss, plane_rs, line_ss, line_rs,
    sl_ss, sl_rs, sp_ss, sp_rs, sc_ss, sc_rs,
    ml_ss, ml_rs, mp_ss, mp_rs, mc_ss, mc_rs, ul_ss, ul_rs, up_ss, up_rs, uc_ss, uc_rs,
):
    A, Y, S, X = sizes
    rows, width = master.shape
    a = lax.axis_index("gx")
    gy = lax.axis_index("gy")
    x = lax.axis_index("gz")
    y, c = gy // S, gy % S

    def device(a_, y_, c_, x_):
        return (a_, y_ * S + c_, x_)

    def remote(src, dst, ss, rs, where):
        return pltpu.make_async_remote_copy(
            src_ref=src, dst_ref=dst, send_sem=ss, recv_sem=rs, device_id=device(*where), device_id_type=MESH
        )

    plane = [q for q in itertools.product(range(Y), range(X)) if q != (0, 0)]
    lines_far = list(range(A - 1, 0, -1))
    lines_near = list(range(1, A))
    others = [(d, 0, 0, 0) for d in lines_far] + [(0, dy, 0, dx) for dy, dx in plane] + [(0, 0, k, 0) for k in range(1, S)]

    def at(da, dy, dc, dx, sign=1):
        return (offset(a, da, A, sign), offset(y, dy, Y, sign), offset(c, dc, S, sign), offset(x, dx, X, sign))

    barrier = pltpu.get_barrier_semaphore()
    for o in others:
        pl.semaphore_signal(barrier, inc=1, device_id=device(*at(*o)), device_id_type=MESH)

    loads_own, loads_far = {}, {}
    order = lines_far + [0]
    for d in order:
        target = offset(a, d, A)
        for k in range(1, S):
            loads_far[d, k] = pltpu.make_async_copy(
                grads.at[target, :, offset(c, k, S)], far_half.at[k - 1, d], load_far.at[k - 1, d]
            )
            loads_far[d, k].start()
    for d in order:
        target = offset(a, d, A)
        loads_own[d] = pltpu.make_async_copy(grads.at[target, :, c], own_half.at[d], load_own.at[d])
        loads_own[d].start()
    loads_small = [
        pltpu.make_async_copy(src, dst, load_small.at[i])
        for i, (src, dst) in enumerate(((master, m_in), (first, f_in), (second, s_in)))
    ]
    for copy in loads_small:
        copy.start()

    pl.semaphore_wait(barrier, len(others))

    own = (a, y, c, x)

    class Gather:
        def __init__(self, ref, line_sems, plane_sems, core_sems):
            self.ref, self.line_sems, self.plane_sems, self.core_sems = ref, line_sems, plane_sems, core_sems
            self.line, self.plane, self.core = {}, {}, {}

        def copy(self, block, sems, slot, where):
            ref = self.ref.at[block]
            hop = remote(ref, ref, sems[0].at[slot], sems[1].at[slot], at(*where))
            hop.start()
            return hop

        def to_line(self):
            for d in lines_far:
                self.line[d] = self.copy(own, self.line_sems, d - 1, (d, 0, 0, 0))

        def to_plane(self, d):
            for i, (dy, dx) in enumerate(plane):
                self.plane[d, i] = self.copy(at(d, 0, 0, 0, -1), self.plane_sems, (d, i), (0, dy, 0, dx))

        def to_core(self, d, i):
            dy, dx = plane[i] if i < len(plane) else (0, 0)
            for k in range(1, S):
                self.core[d, i, k] = self.copy(at(d, dy, 0, dx, -1), self.core_sems, (k - 1, d, i), (0, 0, k, 0))

        def relay_line(self, d):
            self.line[d].wait_recv()
            self.to_plane(d)
            self.to_core(d, len(plane))

        def relay_plane(self, d):
            for i in range(len(plane)):
                self.plane[d, i].wait_recv()
                self.to_core(d, i)

        def finish(self):
            for hop in self.core.values():
                hop.wait_recv()
            for group in (self.line, self.plane, self.core):
                for hop in group.values():
                    hop.wait_send()

    of_master = Gather(all_master, (ml_ss, ml_rs), (mp_ss, mp_rs), (mc_ss, mc_rs))
    of_update = Gather(all_update, (ul_ss, ul_rs), (up_ss, up_rs), (uc_ss, uc_rs))

    pair = {}
    for d in order:
        for k in range(1, S):
            loads_far[d, k].wait()
            pair[d, k] = remote(
                far_half.at[k - 1, d], pair_recv.at[k - 1, d], pair_ss.at[k - 1, d], pair_rs.at[k - 1, d], at(0, 0, k, 0)
            )
            pair[d, k].start()

    ids_row = jnp.broadcast_to(ids[...], (rows, rows)).astype(jnp.float32)
    diagonal = lax.broadcasted_iota(jnp.int32, (rows, rows), 0) == lax.broadcasted_iota(jnp.int32, (rows, rows), 1)
    ids_col = jnp.sum(jnp.where(diagonal, ids_row, 0.0), axis=1, keepdims=True)
    lane = lax.broadcasted_iota(jnp.int32, (rows, 128), 1).astype(jnp.float32)
    hit_w, hit_u, hit_n = lane == ids_col, lane == ids_col + NT, lane == ids_col + 2 * NT
    for copy in loads_small:
        copy.wait()
    weights = m_in[...]
    all_master[own] = weights.astype(jnp.bfloat16)
    of_master.to_line()
    of_master.to_plane(0)
    of_master.to_core(0, len(plane))
    weight_rows = jnp.sum(weights * weights, axis=1, keepdims=True)
    fixed_sums = jnp.where(hit_w, weight_rows, 0.0) + jnp.where(hit_n, float(width), 0.0)

    crossing = {}
    for d in order:
        loads_own[d].wait()
        for k in range(1, S):
            pair[d, k].wait_recv()
        for i, (dy, dx) in enumerate(plane):
            y_, x_ = offset(y, dy, Y), offset(x, dx, X)
            total = own_half[d, y_, x_].astype(jnp.float32)
            for k in range(1, S):
                total = total + pair_recv[k - 1, d, y_, x_].astype(jnp.float32)
            pair_send[d, i] = total.astype(jnp.bfloat16)
            crossing[d, i] = remote(
                pair_send.at[d, i], plane_recv.at[d, i], plane_ss.at[d, i], plane_rs.at[d, i], at(0, dy, 0, dx)
            )
            crossing[d, i].start()
        total = own_half[d, y, x].astype(jnp.float32)
        for k in range(1, S):
            total = total + pair_recv[k - 1, d, y, x].astype(jnp.float32)
        acc[d] = total

    along = {}
    for d in order:
        if d == 0:
            for near in lines_near:
                of_master.relay_line(near)
        total = acc[d]
        for i in range(len(plane)):
            crossing[d, i].wait_recv()
            total = total + plane_recv[d, i].astype(jnp.float32)
        if d:
            line_send[d - 1] = total.astype(jnp.bfloat16)
            along[d] = remote(
                line_send.at[d - 1], line_recv.at[d - 1], line_ss.at[d - 1], line_rs.at[d - 1], at(d, 0, 0, 0)
            )
            along[d].start()
    summed = total
    for d in lines_near:
        along[d].wait_recv()
        summed = summed + line_recv[d - 1].astype(jnp.float32)

    new_first = decay_first * f_in[...] + (1.0 - decay_first) * summed
    new_second = decay_second * s_in[...] + (1.0 - decay_second) * summed * summed
    update = new_first / (jnp.sqrt(new_second) + epsilon) + weight_decay * weights
    update_rows = jnp.sum(update * update, axis=1, keepdims=True)
    own_sums = jnp.sum(fixed_sums + jnp.where(hit_u, update_rows, 0.0), axis=0, keepdims=True)
    line_sums[a] = own_sums
    hops = []

    def send_sums(ref, mine, sems, slot, where):
        hops.append(remote(ref.at[mine], ref.at[mine], sems[0].at[slot], sems[1].at[slot], at(*where)))
        hops[-1].start()
        return hops[-1]

    sums_line = [send_sums(line_sums, a, (sl_ss, sl_rs), d - 1, (d, 0, 0, 0)) for d in lines_far]
    all_update[own] = update.astype(jnp.bfloat16)
    of_update.to_line()
    of_update.to_plane(0)
    of_update.to_core(0, len(plane))
    first_out[...] = new_first
    second_out[...] = new_second
    of_master.relay_plane(0)
    for d in lines_near[:-1]:
        of_update.relay_line(d)
    for hop in sums_line:
        hop.wait_recv()
    subtotal = line_sums[0]
    for i in range(1, A):
        subtotal = subtotal + line_sums[i]
    here = y * X + x
    plane_sums[here] = subtotal
    sums_plane = [
        send_sums(plane_sums, here, (sp_ss, sp_rs), i, (0, dy, 0, dx)) for i, (dy, dx) in enumerate(plane)
    ]
    for d in lines_near[-1:]:
        of_update.relay_line(d)
    for d in lines_near:
        of_master.relay_plane(d)
    of_update.relay_plane(0)
    for hop in sums_plane:
        hop.wait_recv()
    subtotal = plane_sums[0]
    for i in range(1, Y * X):
        subtotal = subtotal + plane_sums[i]
    core_sums[c] = subtotal
    sums_core = [send_sums(core_sums, c, (sc_ss, sc_rs), k - 1, (0, 0, k, 0)) for k in range(1, S)]
    for d in lines_near[:-1]:
        of_update.relay_plane(d)
    for hop in sums_core:
        hop.wait_recv()
    totals = core_sums[0]
    for i in range(1, S):
        totals = totals + core_sums[i]
    totals_out[...] = totals
    row_totals = jnp.broadcast_to(totals, (rows, 128))
    row_weight, row_update, row_count = (
        jnp.sum(jnp.where(hit, row_totals, 0.0), axis=1, keepdims=True) for hit in (hit_w, hit_u, hit_n)
    )
    trust = jnp.sqrt(row_weight / (row_update + row_count))
    scaled = trust * update
    m_out[...] = weights - step_size * scaled
    u_out[...] = scaled
    for d in lines_near[-1:]:
        of_update.relay_plane(d)
    of_master.finish()
    of_update.finish()
    for group in (pair, crossing, along):
        for copy in group.values():
            copy.wait_send()
    for hop in hops:
        hop.wait_send()


def write_out(sizes, all_master, all_update, totals, *refs):
    A, Y, S, X = sizes
    rows, width = all_master.shape[-2:]
    kept, out_kept, out_params, params, sems, param_sems = refs[:4], refs[4:8], refs[8], refs[9], refs[10], refs[11]
    copies = [pltpu.make_async_copy(kept[i], out_kept[i], sems.at[i]) for i in range(4)]
    for copy in copies:
        copy.start()
    values = totals[...]
    weight_sq, update_sq, counts = (
        [values[:, group * NT + t : group * NT + t + 1] for t in range(NT)] for group in range(3)
    )
    steps = [step_size * jnp.sqrt(weight_sq[t] / (update_sq[t] + counts[t])) for t in range(NT)]
    ends, end = [], 0.0
    for t in range(NT - 1):
        end = end + counts[t]
        ends.append(end)
    row_of = lax.broadcasted_iota(jnp.int32, (rows, 1), 0)
    for i in range(A):
        for j, (y, c, x) in enumerate(itertools.product(range(Y), range(S), range(X))):
            block = i * Y * S * X + j
            place = ((row_of + block * rows) * width).astype(jnp.float32)
            step = jnp.broadcast_to(steps[NT - 1], (rows, 1))
            for t in reversed(range(NT - 1)):
                step = jnp.where(place < ends[t], steps[t], step)
            value = all_master[i, y, c, x].astype(jnp.float32) - step * all_update[i, y, c, x].astype(jnp.float32)
            params[i, y, c, x] = value.astype(jnp.bfloat16)
        copies.append(pltpu.make_async_copy(params.at[i], out_params.at[i], param_sems.at[i]))
        copies[-1].start()
    for copy in copies:
        copy.wait()


def solution(mesh):
    A, gy, X = mesh.shape["gx"], mesh.shape["gy"], mesh.shape["gz"]
    S = 2 if gy % 2 == 0 else 1
    Y = gy // S
    total = A * gy * X
    planes = max(Y * X - 1, 1)
    lines = max(A - 1, 1)
    cores = max(S - 1, 1)
    bf16, f32 = jnp.bfloat16, jnp.float32
    dma = pltpu.SemaphoreType.DMA

    def on_device(gradients, master_weights, first_moment, second_moment, tensor_ids):
        rows, width = master_weights.shape
        anywhere = pl.BlockSpec(memory_space=pl.ANY)
        vmem = pltpu.VMEM
        small = jax.ShapeDtypeStruct((rows, width), f32)
        kept_bytes = rows * width * 4 * (total + 4) + 1024 * 1024
        grant = min(LARGEST_GRANT, VMEM_BYTES - kept_bytes)
        outs = pl.pallas_call(
            functools.partial(kernel, (A, Y, S, X)),
            out_shape=(vmem((rows, width), f32),) * 4 + (vmem((A, Y, S, X, rows, width), bf16),) * 2 + (vmem((1, 128), f32),),
            in_specs=[anywhere] * 4 + [pl.BlockSpec(memory_space=vmem)],
            out_specs=(pl.BlockSpec(memory_space=vmem),) * 7,
            scratch_shapes=[
                vmem((A, Y, X, rows, width), bf16),
                vmem((cores, A, Y, X, rows, width), bf16),
                vmem((cores, A, Y, X, rows, width), bf16),
                vmem((A, planes, rows, width), bf16),
                vmem((A, planes, rows, width), bf16),
                vmem((lines, rows, width), bf16),
                vmem((lines, rows, width), bf16),
                vmem((A, rows, width), f32),
                vmem((rows, width), f32),
                vmem((rows, width), f32),
                vmem((rows, width), f32),
                vmem((A, 1, 128), f32),
                vmem((Y * X, 1, 128), f32),
                vmem((S, 1, 128), f32),
                dma((A,)), dma((cores, A)), dma((3,)),
                dma((cores, A)), dma((cores, A)),
                dma((A, planes)), dma((A, planes)),
                dma((lines,)), dma((lines,)),
                dma((lines,)), dma((lines,)), dma((planes,)), dma((planes,)), dma((cores,)), dma((cores,)),
                dma((lines,)), dma((lines,)), dma((A, planes)), dma((A, planes)),
                dma((cores, A, planes + 1)), dma((cores, A, planes + 1)),
                dma((lines,)), dma((lines,)), dma((A, planes)), dma((A, planes)),
                dma((cores, A, planes + 1)), dma((cores, A, planes + 1)),
            ],
            compiler_params=pltpu.CompilerParams(collective_id=0, has_side_effects=True, vmem_limit_bytes=grant),
        )(
            gradients.reshape(A, Y, S, X, rows, width),
            master_weights,
            first_moment,
            second_moment,
            tensor_ids[None, :],
        )
        outs = [pltpu.with_memory_space_constraint(out, vmem) for out in outs]
        written = pl.pallas_call(
            functools.partial(write_out, (A, Y, S, X)),
            out_shape=(small,) * 4 + (jax.ShapeDtypeStruct((A, Y, S, X, rows, width), bf16),),
            in_specs=[pl.BlockSpec(memory_space=vmem)] * 7,
            out_specs=(anywhere,) * 5,
            scratch_shapes=[vmem((A, Y, S, X, rows, width), bf16), dma((4,)), dma((A,))],
            compiler_params=pltpu.CompilerParams(vmem_limit_bytes=grant),
        )(outs[4], outs[5], outs[6], outs[0], outs[1], outs[2], outs[3])
        return (*written[:4], written[4].reshape(total * rows, width))

    axes = ("gx", "gy", "gz")
    return jax.shard_map(
        on_device,
        mesh=mesh,
        in_specs=(P(axes, None, None), P(axes, None), P(axes, None), P(axes, None), P(axes)),
        out_specs=(P(axes, None), P(axes, None), P(axes, None), P(axes, None), P()),
        check_vma=False,
    )
```
